32 devices in a mesh: gx: 4 (over y, x), gy: 2 (over core), gz: 4 (over z).
Axes of the slice: x: 2, y: 2, z: 4, core: 2. Of those that a mesh axis runs over, the one named last changes fastest.
Arguments:
- volume: float32 [512, 128, 512], P('gx', 'gy', 'gz'), may hold values from -6 to 6
Outputs:
- prefix: float32 [512, 128, 512], P('gx', 'gy', 'gz')
- box_sum: float32 [512, 128, 512], P('gx', 'gy', 'gz')
The draws below stay inside these ranges and needn't reach their ends.
All inputs are finite; a program needn't handle non-finite values.
Results may differ from the reference program's by a relative error of at most 0.00055.
Values sent between devices are 32-bit elements; how exact they have to be, the bound alone decides.
A program may use at most 128 MiB of HBM per device.

```python
import math
import jax
import jax.numpy as jnp

NX = 512
NY = 128
NZ = 512


def level_of(own_key, shape, split, least, high):
    factor_of = 1.0
    for axis_at, shards_of in split:
        draws = jax.random.uniform(jax.random.fold_in(jax.random.fold_in(own_key, 6), axis_at), (shards_of,), jnp.float32, least / len(split), high / len(split))
        factor_of = factor_of * jnp.repeat(jnp.exp(draws), shape[axis_at] // shards_of).reshape((-1,) + (1,) * (len(shape) - 1 - axis_at))
    return factor_of


def normal_values(stream_key, dims, deviation, bound, pieces=(), dtype=jnp.bfloat16):
    result = jax.random.normal(stream_key, dims, jnp.float32) * deviation
    if len(pieces) > 0:
        result = level_of(stream_key, dims, pieces, -0.22, 0.18) * result
    return jnp.clip(result, min=-bound, max=bound).astype(dtype)


def setup_inputs(seed: int = 0) -> dict:
    key_of = jax.random.split(jax.random.key(seed), 2)
    volume = normal_values(key_of[0], (NX, NY, NZ), 1.0, 6.0, ((0, 4), (1, 2), (2, 4)), jnp.float32)
    return {"volume": volume}


def reference(volume):
    summed = jnp.cumsum(jnp.cumsum(jnp.cumsum(volume, axis=2), axis=1), axis=0)
    size_x, size_y, size_z = volume.shape
    prefix = summed * jnp.float32(1.0 / math.sqrt(size_x * size_y * size_z))
    padded = jnp.pad(summed, ((3, 0), (3, 0), (3, 0)))
    padded = jnp.pad(padded, ((0, 2), (0, 2), (0, 2)), mode='edge')
    total = jnp.zeros(volume.shape, jnp.float32)
    for first in range(2):
        for second in range(2):
            for third in range(2):
                piece = padded[5 * first:5 * first + size_x, 5 * second:5 * second + size_y, 5 * third:5 * third + size_z]
                if (3 - first - second - third) % 2 == 0:
                    total = total + piece
                else:
                    total = total - piece
    box_sum = total * jnp.float32(1.0 / math.sqrt(125.0))
    return (prefix, box_sum)
```

```python
import functools
import math

import jax
import jax.numpy as jnp
from jax import lax
from jax.experimental import pallas as pl
from jax.experimental.pallas import tpu as pltpu
from jax.sharding import PartitionSpec as P

F32 = jnp.float32
BF16 = jnp.bfloat16
MESH = pl.DeviceIdType.MESH
USED = (0, 2, 3, 4, 5)
PLANES = 16


def split(a, axis):
    hi = a.astype(BF16)
    lo = (a - hi.astype(F32)).astype(BF16)
    return jnp.concatenate([hi, lo], axis=axis)


def source_index(kind, length):
    return {2: length - 2, 3: length - 1, 4: 0, 5: 1}[kind]


def selector(length):
    kind = lax.broadcasted_iota(jnp.int32, (8, length), 0)
    at = lax.broadcasted_iota(jnp.int32, (8, length), 1)
    pick = kind == 0
    for k in (2, 3, 4, 5):
        pick = pick | ((kind == k) & (at == source_index(k, length)))
    one = jnp.where(pick, 1.0, 0.0).astype(BF16)
    return jnp.concatenate([one, one], axis=1)


def z_sources(rows):
    return lax.dot_general(
        selector(rows.shape[1]),
        split(rows, 1),
        (((1,), (1,)), ((), ())),
        preferred_element_type=F32,
    )


def sources_kernel(ny, nz, v_ref, x_ref, y_ref, z_ref, zy_ref, zx_ref, zxy_ref):
    i, steps = pl.program_id(0), pl.num_programs(0)
    nx = steps * PLANES
    blocks = PLANES * ny // 128
    zrows = z_ref.shape[0] // 8

    @pl.when(i == 0)
    def _():
        x_ref[...] = jnp.zeros_like(x_ref)
        y_ref[...] = jnp.zeros_like(y_ref)
        x_ref[4] = v_ref[pl.ds(0, ny), :]
        x_ref[5] = v_ref[pl.ds(ny, ny), :]

    total = v_ref[pl.ds(0, ny), :]
    for x in range(1, PLANES):
        total = total + v_ref[pl.ds(x * ny, ny), :]
    x_ref[0] = x_ref[0] + total
    at = pl.ds(pl.multiple_of(i * PLANES, PLANES), PLANES)
    y_ref[0, at, :] = jnp.sum(v_ref[...].reshape(PLANES, ny, nz), axis=1)
    for k in (2, 3, 4, 5):
        y_ref[k, at, :] = v_ref[pl.ds(source_index(k, ny), PLANES, stride=ny), :]
    found = z_sources(v_ref[...])
    for b in range(blocks):
        z_ref[pl.ds(i * blocks + b, 8, stride=zrows), :] = found[:, b * 128 : (b + 1) * 128]

    @pl.when(i == steps - 1)
    def _():
        x_ref[2] = v_ref[pl.ds((PLANES - 2) * ny, ny), :]
        x_ref[3] = v_ref[pl.ds((PLANES - 1) * ny, ny), :]
        count = y_ref.shape[1] - 8
        planes = x_ref[...]
        y_ref[0, pl.ds(count, 8), :] = jnp.sum(planes, axis=1)
        for k in (2, 3, 4, 5):
            y_ref[k, pl.ds(count, 8), :] = planes[:, source_index(k, ny), :]
        for k in range(8):
            zy_ref[k] = z_sources(y_ref[k, pl.ds(0, count), :])
        pairs = planes.reshape(4, 2 * ny, nz)
        for k in range(4):
            zx_ref[k] = z_sources(pairs[k])
        corner = y_ref[:, pl.ds(count, 8), :].reshape(64, nz)
        zxy_ref[0] = z_sources(jnp.concatenate([corner, jnp.zeros_like(corner)], axis=0))


class Exchange:
    def __init__(self, send, recv):
        self.send, self.recv, self.count = send, recv, 0

    def start(self, axis, shift, src, dst):
        n, me = lax.axis_size(axis), lax.axis_index(axis)
        at = self.count
        self.count += 1
        copy = pltpu.make_async_remote_copy(
            src_ref=src,
            dst_ref=dst,
            send_sem=self.send.at[at],
            recv_sem=self.recv.at[at],
            device_id={axis: lax.rem(me + shift + n, n)},
            device_id_type=MESH,
        )
        sends = (me + shift >= 0) & (me + shift < n)
        receives = (me - shift >= 0) & (me - shift < n)
        pl.when(sends)(copy.start)
        return sends, receives, copy

    def layers(self, axis, src, carry, halo):
        out = []
        n = lax.axis_size(axis)
        if n > 1:
            out.append(self.start(axis, 1, src.at[pl.ds(2, 2)], halo.at[pl.ds(0, 2)]))
            out.append(self.start(axis, -1, src.at[pl.ds(4, 2)], halo.at[pl.ds(2, 2)]))
        for d in range(1, n):
            out.append(self.start(axis, d, src.at[pl.ds(0, 1)], carry.at[pl.ds(d - 1, 1)]))
        return out

    def whole(self, axis, src, slots):
        n = lax.axis_size(axis)
        out = [self.start(axis, d, src, slots.at[d - 1]) for d in range(1, n)]
        if n > 1:
            out.append(self.start(axis, -1, src, slots.at[n - 1]))
        return out


def arrived(copies):
    for _, receives, copy in copies:
        pl.when(receives)(copy.wait_recv)


def sent(copies):
    for sends, _, copy in copies:
        pl.when(sends)(copy.wait_send)


def carry_total(carry, n):
    total = carry[0]
    for d in range(1, n - 1):
        total = total + carry[d]
    return total


def put_layers(out_ref, carry, halo, n):
    out_ref[0] = carry_total(carry, n)
    out_ref[1] = jnp.zeros_like(out_ref[1])
    for k in range(4):
        out_ref[2 + k] = halo[k]
    for k in (6, 7):
        out_ref[k] = jnp.zeros_like(out_ref[k])


def combined(slots, n, kind):
    total = slots[0]
    for d in range(1, n - 1):
        total = total + slots[d]
    zero = jnp.zeros_like(total)
    result = jnp.where(kind == 0, total, zero)
    result = jnp.where((kind == 2) | (kind == 3), slots[0], result)
    return jnp.where((kind == 4) | (kind == 5), slots[n - 1], result)


def exchange_kernel(
    x_in, y_in, z_in, zy_in, zx_in, zxy_in,
    x_out, y_out, z_out, zy_out, zx_out, zxy_out,
    xc, xh, yc, yh, zc, zh, zyc, zyh, zyk, zxc, zxh, corner_y, corner_x_src, corner_x,
    z1_src, z1, z2_src, z2, send, recv,
):
    sizes = {a: lax.axis_size(a) for a in ("gx", "gy", "gz")}
    nx, ny, nz = sizes["gx"], sizes["gy"], sizes["gz"]
    for ref in (xc, xh, yc, yh, zc, zh, zyc, zyh, zxc, zxh, corner_y, corner_x, z1, z2):
        ref[...] = jnp.zeros_like(ref)
    barrier = pltpu.get_barrier_semaphore()
    for axis, n in sizes.items():
        me = lax.axis_index(axis)
        for d in range(1, n):
            pl.semaphore_signal(
                barrier, inc=1, device_id={axis: lax.rem(me + d, n)}, device_id_type=MESH
            )
    pl.semaphore_wait(barrier, nx + ny + nz - 3)

    ex = Exchange(send, recv)
    to_y = ex.layers("gy", y_in, yc, yh)
    to_y += ex.layers("gy", zy_in, zyc, zyh)
    to_y += ex.whole("gy", zxy_in, corner_y)
    to_x = ex.layers("gx", x_in, xc, xh)
    to_x.append(ex.start("gx", 1, zx_in.at[pl.ds(1, 1)], zxh.at[pl.ds(0, 1)]))
    to_x.append(ex.start("gx", -1, zx_in.at[pl.ds(2, 1)], zxh.at[pl.ds(1, 1)]))
    for d in range(1, nx):
        to_x.append(ex.start("gx", d, zx_in.at[pl.ds(0, 1)], zxc.at[pl.ds(d - 1, 1)]))
    to_z = ex.layers("gz", z_in, zc, zh)

    lane = lax.broadcasted_iota(jnp.int32, (1, 8, 128), 2)
    row = lax.broadcasted_iota(jnp.int32, (1, 8, 128), 1)
    arrived(to_y)
    count = y_in.shape[1] - 8
    put_layers(y_out, yc, yh, ny)
    put_layers(zyk, zyc, zyh, ny)
    z1_src[...] = zyk[...]
    more_z = ex.whole("gz", z1_src, z1)
    corner_x_src[pl.ds(0, 8)] = y_out[:, pl.ds(count, 8), :]
    corner_x_src[pl.ds(8, 1)] = combined(corner_y, ny, lane // 8)
    more_x = ex.whole("gx", corner_x_src, corner_x)

    arrived(to_x)
    put_layers(x_out, xc, xh, nx)
    z2_src[pl.ds(0, 1)] = carry_total(zxc, nx)[None]
    z2_src[pl.ds(1, 2)] = zxh[...]
    z2_src[pl.ds(3, 1)] = jnp.zeros((1, 8, 128), F32)
    arrived(more_x)
    got = corner_x.at[:, pl.ds(0, 8)]
    y_out[:, pl.ds(count, 8), :] = combined(got, nx, row)
    z2_src[pl.ds(4, 1)] = combined(corner_x.at[:, pl.ds(8, 1)], nx, lax.rem(lane, 8))
    last_z = ex.whole("gz", z2_src, z2)

    arrived(to_z)
    put_layers(z_out, zc, zh, nz)
    arrived(more_z)
    zy_out[...] = combined(z1, nz, row)
    arrived(last_z)
    zx_out[...] = combined(z2.at[:, pl.ds(0, 4)], nz, row)
    zxy_out[...] = combined(z2.at[:, pl.ds(4, 1)], nz, row)
    sent(to_y + to_x + to_z + more_z + more_x + last_z)


def z_weights(nz):
    rows = lax.broadcasted_iota(jnp.int32, (nz, nz), 0)
    cols = lax.broadcasted_iota(jnp.int32, (nz, nz), 1)
    lower = jnp.where(rows <= cols, 1.0, 0.0).astype(BF16)
    band = jnp.where(jnp.abs(rows - cols) <= 2, 1.0, 0.0).astype(BF16)
    half = jnp.concatenate([lower, band], axis=1)
    kind = lax.broadcasted_iota(jnp.int32, (8, nz), 0)
    at = lax.broadcasted_iota(jnp.int32, (8, nz), 1)
    add = (kind == 2) & (at == 0)
    add |= (kind == 3) & (at <= 1)
    add |= (kind == 4) & (at >= nz - 2)
    add |= (kind == 5) & (at == nz - 1)
    edge = jnp.concatenate(
        [jnp.where(kind == 0, 1.0, 0.0).astype(BF16), jnp.where(add, 1.0, 0.0).astype(BF16)], axis=1
    )
    return jnp.concatenate([half, half], axis=0), jnp.concatenate([edge, edge], axis=0)


def along_z(rows, edges, w_ref, e_ref):
    main = jnp.dot(split(rows, 1), w_ref[...], preferred_element_type=F32)
    return main + lax.dot_general(
        split(edges, 0), e_ref[...], (((0,), (0,)), ((), ())), preferred_element_type=F32
    )


def final_kernel(
    ny, nz, scale,
    v_ref, x_ref, y_ref, z_ref, zy_ref, zx_ref, zxy_ref, w_ref, e_ref,
    prefix_ref, box_ref,
    grid_z, rows_y, plane_z, run, tall, boxed,
):
    i, steps = pl.program_id(0), pl.num_programs(0)
    count = y_ref.shape[1] - 8
    blocks = PLANES * ny // 128
    zrows = z_ref.shape[0] // 8

    def y_prefix(piece, start):
        row = lax.broadcasted_iota(jnp.int32, (1, 8, nz), 1)
        c = piece.reshape(ny // 8, 8, nz)
        for step in (1, 2, 4):
            c = c + jnp.where(row >= step, pltpu.roll(c, step, 1), 0.0)
        out = []
        for k in range(ny // 8):
            out.append(c[k] + start)
            start = out[-1][7:8]
        return jnp.concatenate(out, axis=0)

    def y_box(slot, piece, before, after):
        tall[slot, pl.ds(8, ny), :] = piece
        tall[slot, pl.ds(6, 1), :] = before[0]
        tall[slot, pl.ds(7, 1), :] = before[1]
        tall[slot, pl.ds(8 + ny, 1), :] = after[0]
        tall[slot, pl.ds(9 + ny, 1), :] = after[1]
        total = piece
        for d in (6, 7, 9, 10):
            total = total + tall[slot, pl.ds(d, ny), :]
        return total

    def row_of(k, x, part):
        return rows_y[k, pl.ds(x, 1), pl.ds(part * nz, nz)]

    @pl.when(i == 0)
    def _():
        for k in USED:
            rows_y[k, pl.ds(0, count), :] = along_z(
                y_ref[k, pl.ds(0, count), :], zy_ref[k], w_ref, e_ref
            )
        corner = along_z(
            y_ref[:, pl.ds(count, 8), :].reshape(64, nz), zxy_ref[0][:, :64], w_ref, e_ref
        )
        rows_y[:, pl.ds(count, 8), :] = corner.reshape(8, 8, 2 * nz)
        edges = jnp.concatenate([zx_ref[k] for k in range(4)], axis=1)
        plane_z[...] = along_z(x_ref[...].reshape(8 * ny, nz), edges, w_ref, e_ref)
        run[...] = y_prefix(plane_z[pl.ds(0, ny), pl.ds(0, nz)], row_of(0, count, 0))
        for k, to in ((2, 0), (3, 1), (4, count + 2), (5, count + 3)):
            boxed[to] = y_box(
                k % 4,
                plane_z[pl.ds(k * ny, ny), pl.ds(nz, nz)],
                [row_of(t, count + k, 1) for t in (2, 3)],
                [row_of(t, count + k, 1) for t in (4, 5)],
            )

    @pl.when(i < steps - 1)
    def _():
        edges = jnp.concatenate(
            [z_ref[pl.ds(i * blocks + b, 8, stride=zrows), :] for b in range(blocks)], axis=1
        )
        grid_z[...] = along_z(v_ref[...], edges, w_ref, e_ref)
        running = run[...]
        here = pl.ds(pl.multiple_of(i * PLANES, PLANES), PLANES)
        starts = rows_y[0, here, pl.ds(0, nz)]
        sides = {t: rows_y[t, here, pl.ds(nz, nz)] for t in (2, 3, 4, 5)}
        for p in range(PLANES):
            x = i * PLANES + p
            at = pl.ds(p * ny, ny)
            running = running + y_prefix(grid_z[at, pl.ds(0, nz)], starts[p : p + 1])
            prefix_ref[at, :] = running * F32(scale)
            boxed[x + 2] = y_box(
                p % 4,
                grid_z[at, pl.ds(nz, nz)],
                [sides[t][p : p + 1] for t in (2, 3)],
                [sides[t][p : p + 1] for t in (4, 5)],
            )
        run[...] = running

    @pl.when(i > 0)
    def _():
        for p in range(PLANES):
            x = (i - 1) * PLANES + p
            total = boxed[x]
            for d in range(1, 5):
                total = total + boxed[x + d]
            box_ref[pl.ds(p * ny, ny), :] = total * F32(1.0 / math.sqrt(125.0))


def fixed(*shape):
    return pl.BlockSpec(shape, lambda i: (0,) * len(shape))


def per_device(volume):
    cx, cy, cz = volume.shape
    nx, ny, nz = (lax.axis_size(a) for a in ("gx", "gy", "gz"))
    steps = cx // PLANES
    rows = PLANES * cy
    zrows = cx * cy // 128
    flat = volume.reshape(cx * cy, cz)

    def of(*shape):
        return jax.ShapeDtypeStruct(shape, F32)

    faces = [(8, cy, cz), (8, cx + 8, cz), (8 * zrows, 128), (8, 8, cx), (4, 8, 2 * cy), (1, 8, 128)]
    x, y, z, zy, zx, zxy = pl.pallas_call(
        functools.partial(sources_kernel, cy, cz),
        grid=(steps,),
        in_specs=[pl.BlockSpec((rows, cz), lambda i: (i, 0))],
        out_specs=[fixed(*s) for s in faces],
        out_shape=[of(*s) for s in faces],
    )(flat)

    z = z.reshape(8, zrows, 128)
    vmem = pl.BlockSpec(memory_space=pltpu.VMEM)
    sent_shapes = [a.shape for a in (x, y, z, zy, zx, zxy)]
    copies = 4 * (nx + ny + nz) + 4
    lx, ly, lz = (max(n - 1, 1) for n in (nx, ny, nz))
    buffers = [
        (lx, cy, cz), (4, cy, cz),
        (ly, cx + 8, cz), (4, cx + 8, cz),
        (lz, zrows, 128), (4, zrows, 128),
        (ly, 8, cx), (4, 8, cx), (8, 8, cx),
        (lx, 8, 128), (2, 8, 128),
        (ny, 1, 8, 128),
        (9, 8, 128), (nx, 9, 8, 128),
        (8, 8, 128), (nz, 8, 8, 128),
        (5, 8, 128), (nz, 5, 8, 128),
    ]
    x, y, z, zy, zx, zxy = pl.pallas_call(
        exchange_kernel,
        in_specs=[vmem] * 6,
        out_specs=[vmem] * 6,
        out_shape=[of(*s) for s in sent_shapes],
        scratch_shapes=[pltpu.VMEM(s, F32) for s in buffers]
        + [pltpu.SemaphoreType.DMA((copies,)), pltpu.SemaphoreType.DMA((copies,))],
        compiler_params=pltpu.CompilerParams(collective_id=0, has_side_effects=True),
    )(x, y, z, zy, zx, zxy)
    z = z.reshape(8 * zrows, 128)

    weights, edge_weights = z_weights(cz)
    scale = 1.0 / math.sqrt(cx * nx * cy * ny * cz * nz)
    prefix, box = pl.pallas_call(
        functools.partial(final_kernel, cy, cz, scale),
        grid=(steps + 1,),
        in_specs=[pl.BlockSpec((rows, cz), lambda i: (jnp.minimum(i, steps - 1), 0))]
        + [fixed(*a.shape) for a in (x, y, z, zy, zx, zxy, weights, edge_weights)],
        out_specs=[
            pl.BlockSpec((rows, cz), lambda i: (jnp.minimum(i, steps - 1), 0)),
            pl.BlockSpec((rows, cz), lambda i: (jnp.maximum(i - 1, 0), 0)),
        ],
        out_shape=[of(cx * cy, cz), of(cx * cy, cz)],
        scratch_shapes=[
            pltpu.VMEM((rows, 2 * cz), F32),
            pltpu.VMEM((8, cx + 8, 2 * cz), F32),
            pltpu.VMEM((8 * cy, 2 * cz), F32),
            pltpu.VMEM((cy, cz), F32),
            pltpu.VMEM((4, cy + 16, cz), F32),
            pltpu.VMEM((cx + 4, cy, cz), F32),
        ],
        compiler_params=pltpu.CompilerParams(vmem_limit_bytes=48 * 1024 * 1024),
    )(flat, x, y, z, zy, zx, zxy, weights, edge_weights)
    return prefix.reshape(cx, cy, cz), box.reshape(cx, cy, cz)


def solution(mesh):
    return jax.shard_map(
        per_device,
        mesh=mesh,
        in_specs=(P("gx", "gy", "gz"),),
        out_specs=(P("gx", "gy", "gz"), P("gx", "gy", "gz")),
        check_vma=False,
    )
```

```python
import functools
import math

import jax
import jax.numpy as jnp
from jax import lax
from jax.experimental import pallas as pl
from jax.experimental.pallas import tpu as pltpu
from jax.sharding import PartitionSpec as P

F32 = jnp.float32
BF16 = jnp.bfloat16
MESH = pl.DeviceIdType.MESH
USED = (0, 2, 3, 4, 5)
PLANES = 32
CHUNKS = 4


def split(a, axis):
    hi = a.astype(BF16)
    lo = (a - hi.astype(F32)).astype(BF16)
    return jnp.concatenate([hi, lo], axis=axis)


def source_index(kind, length):
    return {2: length - 2, 3: length - 1, 4: 0, 5: 1}[kind]


def selector(length):
    kind = lax.broadcasted_iota(jnp.int32, (8, length), 0)
    at = lax.broadcasted_iota(jnp.int32, (8, length), 1)
    pick = kind == 0
    for k in (2, 3, 4, 5):
        pick = pick | ((kind == k) & (at == source_index(k, length)))
    one = jnp.where(pick, 1.0, 0.0).astype(BF16)
    return jnp.concatenate([one, one], axis=1)


def z_sources(rows):
    return lax.dot_general(
        selector(rows.shape[1]),
        split(rows, 1),
        (((1,), (1,)), ((), ())),
        preferred_element_type=F32,
    )


class Exchange:
    def __init__(self, send, recv):
        self.send, self.recv, self.count = send, recv, 0

    def start(self, axis, shift, src, dst):
        n, me = lax.axis_size(axis), lax.axis_index(axis)
        at = self.count
        self.count += 1
        copy = pltpu.make_async_remote_copy(
            src_ref=src,
            dst_ref=dst,
            send_sem=self.send.at[at],
            recv_sem=self.recv.at[at],
            device_id={axis: lax.rem(me + shift + n, n)},
            device_id_type=MESH,
        )
        sends = (me + shift >= 0) & (me + shift < n)
        receives = (me - shift >= 0) & (me - shift < n)
        pl.when(sends)(copy.start)
        return sends, receives, copy

    def layers(self, axis, src, carry, halo):
        out = []
        n = lax.axis_size(axis)
        if n > 1:
            out.append(self.start(axis, 1, src.at[pl.ds(2, 2)], halo.at[pl.ds(0, 2)]))
            out.append(self.start(axis, -1, src.at[pl.ds(4, 2)], halo.at[pl.ds(2, 2)]))
        for d in range(1, n):
            out.append(self.start(axis, d, src.at[pl.ds(0, 1)], carry.at[pl.ds(d - 1, 1)]))
        return out

    def whole(self, axis, src, slots):
        n = lax.axis_size(axis)
        out = [self.start(axis, d, src, slots.at[d - 1]) for d in range(1, n)]
        if n > 1:
            out.append(self.start(axis, -1, src, slots.at[n - 1]))
        return out


def arrived(copies):
    for _, receives, copy in copies:
        pl.when(receives)(copy.wait_recv)


def sent(copies):
    for sends, _, copy in copies:
        pl.when(sends)(copy.wait_send)


def carry_total(carry, n):
    total = carry[0]
    for d in range(1, n - 1):
        total = total + carry[d]
    return total


def put_layers(out_ref, carry, halo, n):
    out_ref[0] = carry_total(carry, n)
    out_ref[1] = jnp.zeros_like(out_ref[1])
    for k in range(4):
        out_ref[2 + k] = halo[k]
    for k in (6, 7):
        out_ref[k] = jnp.zeros_like(out_ref[k])


def combined(slots, n, kind):
    total = slots[0]
    for d in range(1, n - 1):
        total = total + slots[d]
    zero = jnp.zeros_like(total)
    result = jnp.where(kind == 0, total, zero)
    result = jnp.where((kind == 2) | (kind == 3), slots[0], result)
    return jnp.where((kind == 4) | (kind == 5), slots[n - 1], result)


def exchange_kernel(
    volume,
    v, x_out, y_out, xy_out, z_out, z1_out, z2_out,
    x_src, y_src, z_src, s_src, zx_src, corner, xx_src, corner_x, z1_src, z2_src,
    xc, xh, yc, yh, zc, zh, sc, sh, small, zxc, zxh, corner_y_in, xxc, xxh, corner_x_in,
    z1c, z1h, z2c, z2h, local, send, recv,
):
    sizes = {a: lax.axis_size(a) for a in ("gx", "gy", "gz")}
    nx, ny, nz = sizes["gx"], sizes["gy"], sizes["gz"]
    cx, cy, cz = v.shape
    part = cx // CHUNKS
    loads = []
    for c in range(CHUNKS):
        at = pl.ds(c * part, part)
        loads.append(pltpu.make_async_copy(volume.at[at], v.at[at], local.at[c]))
        loads[-1].start()
    for ref in (xc, xh, yc, yh, zc, zh, sc, sh, zxc, zxh, corner_y_in, xxc, xxh, corner_x_in,
                z1c, z1h, z2c, z2h):
        ref[...] = jnp.zeros_like(ref)
    barrier = pltpu.get_barrier_semaphore()
    for axis, n in sizes.items():
        me = lax.axis_index(axis)
        for d in range(1, n):
            pl.semaphore_signal(
                barrier, inc=1, device_id={axis: lax.rem(me + d, n)}, device_id_type=MESH
            )

    x_src[...] = jnp.zeros_like(x_src)
    s_src[...] = jnp.zeros_like(s_src)
    total = None
    for c in range(CHUNKS):
        at = pl.ds(c * part, part)
        loads[c].wait()
        planes = v[at]
        partial = jnp.sum(planes, axis=0)
        total = partial if total is None else total + partial
        y_src[0, at, :] = jnp.sum(planes, axis=1)
        for k in (2, 3, 4, 5):
            y_src[k, at, :] = planes[:, source_index(k, cy), :]
    x_src[0] = total
    for k in (2, 3, 4, 5):
        x_src[k] = v[source_index(k, cx)]
    pl.semaphore_wait(barrier, nx + ny + nz - 3)

    ex = Exchange(send, recv)
    to_y = ex.layers("gy", y_src, yc, yh)
    to_x = ex.layers("gx", x_src, xc, xh)
    blocks = part * cy // 128
    for c in range(CHUNKS):
        found = z_sources(v[pl.ds(c * part, part)].reshape(part * cy, cz))
        z_src[:, pl.ds(c * blocks, blocks), :] = found.reshape(8, blocks, 128)
    to_z = ex.layers("gz", z_src, zc, zh)

    planes = x_src[...]
    for k in USED:
        rows = jnp.sum(planes, axis=1) if k == 0 else planes[:, source_index(k, cy), :]
        s_src[k, pl.ds(0, 8), :] = rows
    zero = jnp.zeros((64, cz), F32)
    rows = [y_src[k] for k in USED] + [planes[:6].reshape(6 * cy, cz)]
    rows += [s_src[:, k, :] for k in range(8)] + [zero]
    found = z_sources(jnp.concatenate(rows, axis=0))
    for at, k in enumerate(USED):
        s_src[k, pl.ds(8, 8), :] = found[:, at * 128 : (at + 1) * 128]
    for k in range(3):
        zx_src[k] = found[:, (5 + k) * 128 : (6 + k) * 128]
    corner[0] = found[:, 8 * 128 : 9 * 128]
    to_y += ex.layers("gy", s_src, sc, sh)
    to_y += ex.whole("gy", corner, corner_y_in)
    to_x.append(ex.start("gx", 1, zx_src.at[pl.ds(1, 1)], zxh.at[pl.ds(0, 1)]))
    to_x.append(ex.start("gx", -1, zx_src.at[pl.ds(2, 1)], zxh.at[pl.ds(1, 1)]))
    for d in range(1, nx):
        to_x.append(ex.start("gx", d, zx_src.at[pl.ds(0, 1)], zxc.at[pl.ds(d - 1, 1)]))

    lane = lax.broadcasted_iota(jnp.int32, (1, 8, 128), 2)
    arrived(to_y)
    put_layers(small, sc, sh, ny)
    for k in range(8):
        xx_src[k] = small[:, k, :]
        z1_src[k] = small[:, 8 + k, :]
    corner_x[...] = combined(corner_y_in, ny, lax.rem(lane, 8))
    to_x += ex.layers("gx", xx_src, xxc, xxh)
    to_x += ex.whole("gx", corner_x, corner_x_in)
    to_z += ex.layers("gz", z1_src, z1c, z1h)
    put_layers(y_out, yc, yh, ny)

    arrived(to_x)
    pairs = [carry_total(zxc, nx), zxh[0], zxh[1], combined(corner_x_in, nx, lane // 8)[0]]
    for k in range(8):
        rows = [p[k : k + 1] for p in pairs] + [jnp.zeros((4, 128), F32)]
        z2_src[k] = jnp.concatenate(rows, axis=0)
    to_z += ex.layers("gz", z2_src, z2c, z2h)
    put_layers(x_out, xc, xh, nx)
    put_layers(xy_out, xxc, xxh, nx)

    arrived(to_z)
    put_layers(z_out, zc, zh, nz)
    put_layers(z1_out, z1c, z1h, nz)
    put_layers(z2_out, z2c, z2h, nz)
    sent(to_y + to_x + to_z)


def z_weights(nz):
    rows = lax.broadcasted_iota(jnp.int32, (nz, nz), 0)
    cols = lax.broadcasted_iota(jnp.int32, (nz, nz), 1)
    lower = jnp.where(rows <= cols, 1.0, 0.0).astype(BF16)
    band = jnp.where(jnp.abs(rows - cols) <= 2, 1.0, 0.0).astype(BF16)
    half = jnp.concatenate([lower, band], axis=1)
    kind = lax.broadcasted_iota(jnp.int32, (8, nz), 0)
    at = lax.broadcasted_iota(jnp.int32, (8, nz), 1)
    add = (kind == 2) & (at == 0)
    add |= (kind == 3) & (at <= 1)
    add |= (kind == 4) & (at >= nz - 2)
    add |= (kind == 5) & (at == nz - 1)
    edge = jnp.concatenate(
        [jnp.where(kind == 0, 1.0, 0.0).astype(BF16), jnp.where(add, 1.0, 0.0).astype(BF16)], axis=1
    )
    return jnp.concatenate([half, half], axis=0), jnp.concatenate([edge, edge], axis=0)


def along_z(rows, edges, w_ref, e_ref):
    main = jnp.dot(split(rows, 1), w_ref[...], preferred_element_type=F32)
    return main + lax.dot_general(
        split(edges, 0), e_ref[...], (((0,), (0,)), ((), ())), preferred_element_type=F32
    )


def final_kernel(
    ny, nz, scale,
    v_ref, x_ref, y_ref, xy_ref, z_ref, z1_ref, z2_ref, w_ref, e_ref,
    prefix_ref, box_ref,
    grid_z, rows_y, plane_z, corner_z, run, tall, boxed,
):
    i, steps = pl.program_id(0), pl.num_programs(0)
    count = y_ref.shape[1]
    blocks = PLANES * ny // 128
    zrows = z_ref.shape[0] // 8

    def y_prefix(piece, start):
        row = lax.broadcasted_iota(jnp.int32, (1, 8, nz), 1)
        c = piece.reshape(ny // 8, 8, nz)
        for step in (1, 2, 4):
            c = c + jnp.where(row >= step, pltpu.roll(c, step, 1), 0.0)
        out = []
        for k in range(ny // 8):
            out.append(c[k] + start)
            start = out[-1][7:8]
        return jnp.concatenate(out, axis=0)

    def y_box(slot, piece, before, after):
        tall[slot, pl.ds(8, ny), :] = piece
        tall[slot, pl.ds(6, 1), :] = before[0]
        tall[slot, pl.ds(7, 1), :] = before[1]
        tall[slot, pl.ds(8 + ny, 1), :] = after[0]
        tall[slot, pl.ds(9 + ny, 1), :] = after[1]
        total = piece
        for d in (6, 7, 9, 10):
            total = total + tall[slot, pl.ds(d, ny), :]
        return total

    def row_of(k, x, part):
        return corner_z[pl.ds(x * 8 + k, 1), pl.ds(part * nz, nz)]

    @pl.when(i == 0)
    def _():
        for k in USED:
            rows_y[k] = along_z(y_ref[k], z1_ref[:, k, :], w_ref, e_ref)
        corner_z[...] = along_z(xy_ref[...].reshape(64, nz), z2_ref[:, 3, :][:, :64], w_ref, e_ref)
        edges = jnp.concatenate([z2_ref[:, k, :] for k in range(3)], axis=1)
        plane_z[...] = along_z(x_ref[:6].reshape(6 * ny, nz), edges, w_ref, e_ref)
        run[...] = y_prefix(plane_z[pl.ds(0, ny), pl.ds(0, nz)], row_of(0, 0, 0))
        for k, to in ((2, 0), (3, 1), (4, count + 2), (5, count + 3)):
            boxed[to] = y_box(
                k % 4,
                plane_z[pl.ds(k * ny, ny), pl.ds(nz, nz)],
                [row_of(t, k, 1) for t in (2, 3)],
                [row_of(t, k, 1) for t in (4, 5)],
            )

    @pl.when(i < steps - 1)
    def _():
        edges = jnp.concatenate(
            [z_ref[pl.ds(i * blocks + b, 8, stride=zrows), :] for b in range(blocks)], axis=1
        )
        grid_z[...] = along_z(v_ref[pl.ds(i * PLANES * ny, PLANES * ny), :], edges, w_ref, e_ref)
        running = run[...]
        here = pl.ds(pl.multiple_of(i * PLANES, PLANES), PLANES)
        starts = rows_y[0, here, pl.ds(0, nz)]
        sides = {t: rows_y[t, here, pl.ds(nz, nz)] for t in (2, 3, 4, 5)}
        for p in range(PLANES):
            x = i * PLANES + p
            at = pl.ds(p * ny, ny)
            running = running + y_prefix(grid_z[at, pl.ds(0, nz)], starts[p : p + 1])
            prefix_ref[at, :] = running * F32(scale)
            boxed[x + 2] = y_box(
                p % 4,
                grid_z[at, pl.ds(nz, nz)],
                [sides[t][p : p + 1] for t in (2, 3)],
                [sides[t][p : p + 1] for t in (4, 5)],
            )
        run[...] = running

    @pl.when(i > 0)
    def _():
        for p in range(PLANES):
            x = (i - 1) * PLANES + p
            total = boxed[x]
            for d in range(1, 5):
                total = total + boxed[x + d]
            box_ref[pl.ds(p * ny, ny), :] = total * F32(1.0 / math.sqrt(125.0))


def per_device(volume):
    cx, cy, cz = volume.shape
    nx, ny, nz = (lax.axis_size(a) for a in ("gx", "gy", "gz"))
    steps = cx // PLANES
    rows = PLANES * cy
    zrows = cx * cy // 128

    def of(*shape):
        return jax.ShapeDtypeStruct(shape, F32)

    vmem = pl.BlockSpec(memory_space=pltpu.VMEM)
    copies = 8 * (nx + ny + nz) + 4
    lx, ly, lz = (max(n - 1, 1) for n in (nx, ny, nz))
    row = (8, 128)
    faces = [(cx, cy, cz), (8, cy, cz), (8, cx, cz), (8, 8, cz), (8, zrows, 128), (8, 8, cx), (8, 8, 128)]
    buffers = [
        (8, cy, cz), (8, cx, cz), (8, zrows, 128), (8, 16, 128), (3, *row),
        (1, *row), (8, *row), (1, *row), (8, *row), (8, *row),
        (lx, cy, cz), (4, cy, cz), (ly, cx, cz), (4, cx, cz), (lz, zrows, 128), (4, zrows, 128),
        (ly, 16, 128), (4, 16, 128), (8, 16, 128), (lx, *row), (2, *row), (ny, 1, *row),
        (lx, *row), (4, *row), (nx, 1, *row),
        (lz, *row), (4, *row), (lz, *row), (4, *row),
    ]
    held, x, y, xy, z, z1, z2 = pl.pallas_call(
        exchange_kernel,
        in_specs=[pl.BlockSpec(memory_space=pltpu.HBM)],
        out_specs=[vmem] * 7,
        out_shape=[of(*s) for s in faces],
        scratch_shapes=[pltpu.VMEM(s, F32) for s in buffers]
        + [pltpu.SemaphoreType.DMA((CHUNKS,))]
        + [pltpu.SemaphoreType.DMA((copies,)), pltpu.SemaphoreType.DMA((copies,))],
        compiler_params=pltpu.CompilerParams(
            collective_id=0, has_side_effects=True, vmem_limit_bytes=46 * 1024 * 1024
        ),
    )(volume)
    z = z.reshape(8 * zrows, 128)

    weights, edge_weights = z_weights(cz)
    scale = 1.0 / math.sqrt(cx * nx * cy * ny * cz * nz)
    prefix, box = pl.pallas_call(
        functools.partial(final_kernel, cy, cz, scale),
        grid=(steps + 1,),
        in_specs=[vmem] * 9,
        out_specs=[
            pl.BlockSpec((rows, cz), lambda i: (jnp.minimum(i, steps - 1), 0)),
            pl.BlockSpec((rows, cz), lambda i: (jnp.maximum(i - 1, 0), 0)),
        ],
        out_shape=[of(cx * cy, cz), of(cx * cy, cz)],
        scratch_shapes=[
            pltpu.VMEM((rows, 2 * cz), F32),
            pltpu.VMEM((6, cx, 2 * cz), F32),
            pltpu.VMEM((6 * cy, 2 * cz), F32),
            pltpu.VMEM((64, 2 * cz), F32),
            pltpu.VMEM((cy, cz), F32),
            pltpu.VMEM((4, cy + 16, cz), F32),
            pltpu.VMEM((cx + 4, cy, cz), F32),
        ],
        compiler_params=pltpu.CompilerParams(vmem_limit_bytes=24 * 1024 * 1024),
    )(held.reshape(cx * cy, cz), x, y, xy, z, z1, z2, weights, edge_weights)
    return prefix.reshape(cx, cy, cz), box.reshape(cx, cy, cz)


def solution(mesh):
    return jax.shard_map(
        per_device,
        mesh=mesh,
        in_specs=(P("gx", "gy", "gz"),),
        out_specs=(P("gx", "gy", "gz"), P("gx", "gy", "gz")),
        check_vma=False,
    )
```

```python
import functools
import math

import jax
import jax.numpy as jnp
from jax import lax
from jax.experimental import pallas as pl
from jax.experimental.pallas import tpu as pltpu
from jax.sharding import PartitionSpec as P

F32 = jnp.float32
BF16 = jnp.bfloat16
MESH = pl.DeviceIdType.MESH
USED = (0, 2, 3, 4, 5)
PLANES = 32
CHUNKS = 4


def split(a, axis):
    hi = a.astype(BF16)
    lo = (a - hi.astype(F32)).astype(BF16)
    return jnp.concatenate([hi, lo], axis=axis)


def source_index(kind, length):
    return {2: length - 2, 3: length - 1, 4: 0, 5: 1}[kind]


def selector(length):
    kind = lax.broadcasted_iota(jnp.int32, (8, length), 0)
    at = lax.broadcasted_iota(jnp.int32, (8, length), 1)
    pick = kind == 0
    for k in (2, 3, 4, 5):
        pick = pick | ((kind == k) & (at == source_index(k, length)))
    one = jnp.where(pick, 1.0, 0.0).astype(BF16)
    return jnp.concatenate([one, one], axis=1)


def z_sources(rows):
    return lax.dot_general(
        selector(rows.shape[1]),
        split(rows, 1),
        (((1,), (1,)), ((), ())),
        preferred_element_type=F32,
    )


class Exchange:
    def __init__(self, send, recv):
        self.send, self.recv, self.count = send, recv, 0

    def start(self, axis, shift, src, dst):
        n, me = lax.axis_size(axis), lax.axis_index(axis)
        at = self.count
        self.count += 1
        copy = pltpu.make_async_remote_copy(
            src_ref=src,
            dst_ref=dst,
            send_sem=self.send.at[at],
            recv_sem=self.recv.at[at],
            device_id={axis: lax.rem(me + shift + n, n)},
            device_id_type=MESH,
        )
        sends = (me + shift >= 0) & (me + shift < n)
        receives = (me - shift >= 0) & (me - shift < n)
        pl.when(sends)(copy.start)
        return sends, receives, copy

    def layers(self, axis, src, carry, halo):
        out = []
        n = lax.axis_size(axis)
        if n > 1:
            out.append(self.start(axis, 1, src.at[pl.ds(2, 2)], halo.at[pl.ds(0, 2)]))
            out.append(self.start(axis, -1, src.at[pl.ds(4, 2)], halo.at[pl.ds(2, 2)]))
        for d in range(1, n):
            out.append(self.start(axis, d, src.at[pl.ds(0, 1)], carry.at[pl.ds(d - 1, 1)]))
        return out

    def whole(self, axis, src, slots):
        n = lax.axis_size(axis)
        out = [self.start(axis, d, src, slots.at[d - 1]) for d in range(1, n)]
        if n > 1:
            out.append(self.start(axis, -1, src, slots.at[n - 1]))
        return out


def arrived(copies):
    for _, receives, copy in copies:
        pl.when(receives)(copy.wait_recv)


def sent(copies):
    for sends, _, copy in copies:
        pl.when(sends)(copy.wait_send)


def carry_total(carry, n):
    total = carry[0]
    for d in range(1, n - 1):
        total = total + carry[d]
    return total


def put_layers(out_ref, carry, halo, n):
    out_ref[0] = carry_total(carry, n)
    out_ref[1] = jnp.zeros_like(out_ref[1])
    for k in range(4):
        out_ref[2 + k] = halo[k]
    for k in (6, 7):
        out_ref[k] = jnp.zeros_like(out_ref[k])


def combined(slots, n, kind):
    total = slots[0]
    for d in range(1, n - 1):
        total = total + slots[d]
    zero = jnp.zeros_like(total)
    result = jnp.where(kind == 0, total, zero)
    result = jnp.where((kind == 2) | (kind == 3), slots[0], result)
    return jnp.where((kind == 4) | (kind == 5), slots[n - 1], result)


def exchange_kernel(
    volume, w_ref,
    sum_out, box_out, x_out, y_out, xy_out, z_out, z1_out, z2_out,
    v, grid_z, tall, x_src, y_src, z_src, s_src, zx_src, corner, xx_src, corner_x, z1_src, z2_src,
    xc, xh, yc, yh, zc, zh, sc, sh, small, zxc, zxh, corner_y_in, xxc, xxh, corner_x_in,
    z1c, z1h, z2c, z2h, local, send, recv,
):
    sizes = {a: lax.axis_size(a) for a in ("gx", "gy", "gz")}
    nx, ny, nz = sizes["gx"], sizes["gy"], sizes["gz"]
    cx, cy, cz = v.shape
    part = cx // CHUNKS
    loads = []
    for c in range(CHUNKS):
        at = pl.ds(c * part, part)
        loads.append(pltpu.make_async_copy(volume.at[at], v.at[at], local.at[c]))
        loads[-1].start()
    for ref in (xc, xh, yc, yh, zc, zh, sc, sh, zxc, zxh, corner_y_in, xxc, xxh, corner_x_in,
                z1c, z1h, z2c, z2h):
        ref[...] = jnp.zeros_like(ref)
    barrier = pltpu.get_barrier_semaphore()
    for axis, n in sizes.items():
        me = lax.axis_index(axis)
        for d in range(1, n):
            pl.semaphore_signal(
                barrier, inc=1, device_id={axis: lax.rem(me + d, n)}, device_id_type=MESH
            )

    tall[:, pl.ds(0, 8), :] = jnp.zeros((part, 8, cz), F32)
    tall[:, pl.ds(8 + cy, 8), :] = jnp.zeros((part, 8, cz), F32)
    x_src[...] = jnp.zeros_like(x_src)
    s_src[...] = jnp.zeros_like(s_src)
    total = None
    for c in range(CHUNKS):
        at = pl.ds(c * part, part)
        loads[c].wait()
        planes = v[at]
        partial = jnp.sum(planes, axis=0)
        total = partial if total is None else total + partial
        y_src[0, at, :] = jnp.sum(planes, axis=1)
        for k in (2, 3, 4, 5):
            y_src[k, at, :] = planes[:, source_index(k, cy), :]
    x_src[0] = total
    for k in (2, 3, 4, 5):
        x_src[k] = v[source_index(k, cx)]
    pl.semaphore_wait(barrier, nx + ny + nz - 3)

    ex = Exchange(send, recv)
    to_y = ex.layers("gy", y_src, yc, yh)
    to_x = ex.layers("gx", x_src, xc, xh)
    blocks = part * cy // 128
    for c in range(CHUNKS):
        found = z_sources(v[pl.ds(c * part, part)].reshape(part * cy, cz))
        z_src[:, pl.ds(c * blocks, blocks), :] = found.reshape(8, blocks, 128)
    to_z = ex.layers("gz", z_src, zc, zh)

    planes = x_src[...]
    for k in USED:
        rows = jnp.sum(planes, axis=1) if k == 0 else planes[:, source_index(k, cy), :]
        s_src[k, pl.ds(0, 8), :] = rows
    zero = jnp.zeros((64, cz), F32)
    rows = [y_src[k] for k in USED] + [planes[:6].reshape(6 * cy, cz)]
    rows += [s_src[:, k, :] for k in range(8)] + [zero]
    found = z_sources(jnp.concatenate(rows, axis=0))
    for at, k in enumerate(USED):
        s_src[k, pl.ds(8, 8), :] = found[:, at * 128 : (at + 1) * 128]
    for k in range(3):
        zx_src[k] = found[:, (5 + k) * 128 : (6 + k) * 128]
    corner[0] = found[:, 8 * 128 : 9 * 128]
    to_y += ex.layers("gy", s_src, sc, sh)
    to_y += ex.whole("gy", corner, corner_y_in)
    to_x.append(ex.start("gx", 1, zx_src.at[pl.ds(1, 1)], zxh.at[pl.ds(0, 1)]))
    to_x.append(ex.start("gx", -1, zx_src.at[pl.ds(2, 1)], zxh.at[pl.ds(1, 1)]))
    for d in range(1, nx):
        to_x.append(ex.start("gx", d, zx_src.at[pl.ds(0, 1)], zxc.at[pl.ds(d - 1, 1)]))

    def own_sums(c):
        at = pl.ds(c * part, part)
        rows = split(v[at].reshape(part * cy, cz), 1)
        grid_z[...] = jnp.dot(rows, w_ref[...], preferred_element_type=F32)
        row = lax.broadcasted_iota(jnp.int32, (1, 8, cz), 1)
        tiles = grid_z[:, pl.ds(0, cz)].reshape(part * cy // 8, 8, cz)
        for step in (1, 2, 4):
            tiles = tiles + jnp.where(row >= step, pltpu.roll(tiles, step, 1), 0.0)
        tiles = tiles.reshape(part, cy // 8, 8, cz)
        start = None
        for k in range(cy // 8):
            now = tiles[:, k] if k == 0 else tiles[:, k] + start
            sum_out[at, pl.ds(8 * k, 8), :] = now
            start = now[:, 7:8, :]
        main = grid_z[:, pl.ds(cz, cz)].reshape(part, cy, cz)
        tall[:, pl.ds(8, cy), :] = main
        for d in (6, 7, 9, 10):
            main = main + tall[:, pl.ds(d, cy), :]
        box_out[at] = main

    for c in range(CHUNKS // 2):
        own_sums(c)
    lane = lax.broadcasted_iota(jnp.int32, (1, 8, 128), 2)
    arrived(to_y)
    put_layers(small, sc, sh, ny)
    for k in range(8):
        xx_src[k] = small[:, k, :]
        z1_src[k] = small[:, 8 + k, :]
    corner_x[...] = combined(corner_y_in, ny, lax.rem(lane, 8))
    to_x += ex.layers("gx", xx_src, xxc, xxh)
    to_x += ex.whole("gx", corner_x, corner_x_in)
    to_z += ex.layers("gz", z1_src, z1c, z1h)
    put_layers(y_out, yc, yh, ny)
    for c in range(CHUNKS // 2, CHUNKS):
        own_sums(c)

    arrived(to_x)
    pairs = [carry_total(zxc, nx), zxh[0], zxh[1], combined(corner_x_in, nx, lane // 8)[0]]
    for k in range(8):
        rows = [p[k : k + 1] for p in pairs] + [jnp.zeros((4, 128), F32)]
        z2_src[k] = jnp.concatenate(rows, axis=0)
    to_z += ex.layers("gz", z2_src, z2c, z2h)
    put_layers(x_out, xc, xh, nx)
    put_layers(xy_out, xxc, xxh, nx)

    arrived(to_z)
    put_layers(z_out, zc, zh, nz)
    put_layers(z1_out, z1c, z1h, nz)
    put_layers(z2_out, z2c, z2h, nz)
    sent(to_y + to_x + to_z)


def z_weights(nz):
    rows = lax.broadcasted_iota(jnp.int32, (nz, nz), 0)
    cols = lax.broadcasted_iota(jnp.int32, (nz, nz), 1)
    lower = jnp.where(rows <= cols, 1.0, 0.0).astype(BF16)
    band = jnp.where(jnp.abs(rows - cols) <= 2, 1.0, 0.0).astype(BF16)
    half = jnp.concatenate([lower, band], axis=1)
    kind = lax.broadcasted_iota(jnp.int32, (8, nz), 0)
    at = lax.broadcasted_iota(jnp.int32, (8, nz), 1)
    add = (kind == 2) & (at == 0)
    add |= (kind == 3) & (at <= 1)
    add |= (kind == 4) & (at >= nz - 2)
    add |= (kind == 5) & (at == nz - 1)
    edge = jnp.concatenate(
        [jnp.where(kind == 0, 1.0, 0.0).astype(BF16), jnp.where(add, 1.0, 0.0).astype(BF16)], axis=1
    )
    return jnp.concatenate([half, half], axis=0), jnp.concatenate([edge, edge], axis=0)


def y_weights(ny):
    rows = lax.broadcasted_iota(jnp.int32, (128, 128), 0)
    cols = lax.broadcasted_iota(jnp.int32, (128, 128), 1)
    same = rows // ny == cols // ny
    lower = jnp.where(same & (rows <= cols), 1.0, 0.0).astype(BF16)
    band = jnp.where(same & (jnp.abs(rows - cols) <= 2), 1.0, 0.0).astype(BF16)
    half = jnp.concatenate([lower, band], axis=1)
    return jnp.concatenate([half, half], axis=0)


def along_z(rows, edges, w_ref, e_ref):
    main = jnp.dot(split(rows, 1), w_ref[...], preferred_element_type=F32)
    return main + lax.dot_general(
        split(edges, 0), e_ref[...], (((0,), (0,)), ((), ())), preferred_element_type=F32
    )


def final_kernel(
    ny, nz, scale,
    sum_ref, own_ref, x_ref, y_ref, xy_ref, z_ref, z1_ref, z2_ref, w_ref, e_ref, yw_ref,
    prefix_ref, box_ref,
    edge_z, edge_y, rows_y, plane_z, corner_z, run, tall, boxed,
):
    i, steps = pl.program_id(0), pl.num_programs(0)
    count = y_ref.shape[1]
    blocks = PLANES * ny // 128
    zrows = z_ref.shape[0] // 8

    def y_prefix(piece, start):
        row = lax.broadcasted_iota(jnp.int32, (1, 8, nz), 1)
        c = piece.reshape(ny // 8, 8, nz)
        for step in (1, 2, 4):
            c = c + jnp.where(row >= step, pltpu.roll(c, step, 1), 0.0)
        out = []
        for k in range(ny // 8):
            out.append(c[k] + start)
            start = out[-1][7:8]
        return jnp.concatenate(out, axis=0)

    def y_box(slot, piece, before, after):
        tall[slot, pl.ds(8, ny), :] = piece
        tall[slot, pl.ds(6, 1), :] = before[0]
        tall[slot, pl.ds(7, 1), :] = before[1]
        tall[slot, pl.ds(8 + ny, 1), :] = after[0]
        tall[slot, pl.ds(9 + ny, 1), :] = after[1]
        total = piece
        for d in (6, 7, 9, 10):
            total = total + tall[slot, pl.ds(d, ny), :]
        return total

    def row_of(k, x, part):
        return corner_z[pl.ds(x * 8 + k, 1), pl.ds(part * nz, nz)]

    @pl.when(i == 0)
    def _():
        found = jnp.dot(split(z_ref[...], 1), yw_ref[...], preferred_element_type=F32)
        edge_y[pl.ds(0, zrows), :] = found[:zrows, :128]
        edge_y[pl.ds(zrows, 7 * zrows), :] = found[zrows:, 128:]
        for k in USED:
            rows_y[k] = along_z(y_ref[k], z1_ref[:, k, :], w_ref, e_ref)
        corner_z[...] = along_z(xy_ref[...].reshape(64, nz), z2_ref[:, 3, :][:, :64], w_ref, e_ref)
        edges = jnp.concatenate([z2_ref[:, k, :] for k in range(3)], axis=1)
        plane_z[...] = along_z(x_ref[:6].reshape(6 * ny, nz), edges, w_ref, e_ref)
        run[...] = y_prefix(plane_z[pl.ds(0, ny), pl.ds(0, nz)], row_of(0, 0, 0))
        for k, to in ((2, 0), (3, 1), (4, count + 2), (5, count + 3)):
            boxed[to] = y_box(
                k % 4,
                plane_z[pl.ds(k * ny, ny), pl.ds(nz, nz)],
                [row_of(t, k, 1) for t in (2, 3)],
                [row_of(t, k, 1) for t in (4, 5)],
            )

    @pl.when(i < steps - 1)
    def _():
        edges = jnp.concatenate(
            [edge_y[pl.ds(i * blocks + b, 8, stride=zrows), :] for b in range(blocks)], axis=1
        )
        edge_z[...] = lax.dot_general(
            split(edges, 0), e_ref[...], (((0,), (0,)), ((), ())), preferred_element_type=F32
        )
        running = run[...]
        here = pl.ds(pl.multiple_of(i * PLANES, PLANES), PLANES)
        starts = rows_y[0, here, pl.ds(0, nz)]
        b2, b1, a1, a2 = (rows_y[t, here, pl.ds(nz, nz)] for t in (2, 3, 4, 5))
        below, above = b2 + b1, a1 + a2
        row = lax.broadcasted_iota(jnp.int32, (8, nz), 0)
        for p in range(PLANES):
            x = i * PLANES + p
            at = pl.ds(p * ny, ny)
            running = running + (sum_ref[x] + edge_z[at, pl.ds(0, nz)] + starts[p : p + 1])
            prefix_ref[at, :] = running * F32(scale)
            own = own_ref[x] + edge_z[at, pl.ds(nz, nz)]
            low = jnp.where(row == 0, below[p : p + 1], jnp.where(row == 1, b1[p : p + 1], 0.0))
            top = jnp.where(row == 7, above[p : p + 1], jnp.where(row == 6, a1[p : p + 1], 0.0))
            boxed[x + 2, pl.ds(0, 8), :] = own[:8] + low
            boxed[x + 2, pl.ds(8, ny - 16), :] = own[8 : ny - 8]
            boxed[x + 2, pl.ds(ny - 8, 8), :] = own[ny - 8 :] + top
        run[...] = running

    @pl.when(i > 0)
    def _():
        for p in range(PLANES):
            x = (i - 1) * PLANES + p
            total = boxed[x]
            for d in range(1, 5):
                total = total + boxed[x + d]
            box_ref[pl.ds(p * ny, ny), :] = total * F32(1.0 / math.sqrt(125.0))


def per_device(volume):
    cx, cy, cz = volume.shape
    nx, ny, nz = (lax.axis_size(a) for a in ("gx", "gy", "gz"))
    steps = cx // PLANES
    rows = PLANES * cy
    zrows = cx * cy // 128

    def of(*shape):
        return jax.ShapeDtypeStruct(shape, F32)

    vmem = pl.BlockSpec(memory_space=pltpu.VMEM)
    weights, edge_weights = z_weights(cz)
    copies = 8 * (nx + ny + nz) + 4
    lx, ly, lz = (max(n - 1, 1) for n in (nx, ny, nz))
    row = (8, 128)
    faces = [(cx, cy, cz), (cx, cy, cz), (8, cy, cz), (8, cx, cz), (8, 8, cz), (8, zrows, 128), (8, 8, cx), (8, 8, 128)]
    buffers = [
        (cx, cy, cz), (cx // CHUNKS * cy, 2 * cz), (cx // CHUNKS, cy + 16, cz),
        (8, cy, cz), (8, cx, cz), (8, zrows, 128), (8, 16, 128), (3, *row),
        (1, *row), (8, *row), (1, *row), (8, *row), (8, *row),
        (lx, cy, cz), (4, cy, cz), (ly, cx, cz), (4, cx, cz), (lz, zrows, 128), (4, zrows, 128),
        (ly, 16, 128), (4, 16, 128), (8, 16, 128), (lx, *row), (2, *row), (ny, 1, *row),
        (lx, *row), (4, *row), (nx, 1, *row),
        (lz, *row), (4, *row), (lz, *row), (4, *row),
    ]
    own_sum, own_box, x, y, xy, z, z1, z2 = pl.pallas_call(
        exchange_kernel,
        in_specs=[pl.BlockSpec(memory_space=pltpu.HBM), vmem],
        out_specs=[vmem] * 8,
        out_shape=[of(*s) for s in faces],
        scratch_shapes=[pltpu.VMEM(s, F32) for s in buffers]
        + [pltpu.SemaphoreType.DMA((CHUNKS,))]
        + [pltpu.SemaphoreType.DMA((copies,)), pltpu.SemaphoreType.DMA((copies,))],
        compiler_params=pltpu.CompilerParams(
            collective_id=0, has_side_effects=True, vmem_limit_bytes=44 * 1024 * 1024
        ),
    )(volume, weights)
    z = z.reshape(8 * zrows, 128)

    scale = 1.0 / math.sqrt(cx * nx * cy * ny * cz * nz)
    prefix, box = pl.pallas_call(
        functools.partial(final_kernel, cy, cz, scale),
        grid=(steps + 1,),
        in_specs=[vmem] * 11,
        out_specs=[
            pl.BlockSpec((rows, cz), lambda i: (jnp.minimum(i, steps - 1), 0)),
            pl.BlockSpec((rows, cz), lambda i: (jnp.maximum(i - 1, 0), 0)),
        ],
        out_shape=[of(cx * cy, cz), of(cx * cy, cz)],
        scratch_shapes=[
            pltpu.VMEM((rows, 2 * cz), F32),
            pltpu.VMEM((8 * zrows, 128), F32),
            pltpu.VMEM((6, cx, 2 * cz), F32),
            pltpu.VMEM((6 * cy, 2 * cz), F32),
            pltpu.VMEM((64, 2 * cz), F32),
            pltpu.VMEM((cy, cz), F32),
            pltpu.VMEM((4, cy + 16, cz), F32),
            pltpu.VMEM((cx + 4, cy, cz), F32),
        ],
        compiler_params=pltpu.CompilerParams(vmem_limit_bytes=24 * 1024 * 1024),
    )(own_sum, own_box, x, y, xy, z, z1, z2, weights, edge_weights, y_weights(cy))
    return prefix.reshape(cx, cy, cz), box.reshape(cx, cy, cz)


def solution(mesh):
    return jax.shard_map(
        per_device,
        mesh=mesh,
        in_specs=(P("gx", "gy", "gz"),),
        out_specs=(P("gx", "gy", "gz"), P("gx", "gy", "gz")),
        check_vma=False,
    )
```

```python
import functools
import math

import jax
import jax.numpy as jnp
from jax import lax
from jax.experimental import pallas as pl
from jax.experimental.pallas import tpu as pltpu
from jax.sharding import PartitionSpec as P

F32 = jnp.float32
BF16 = jnp.bfloat16
MESH = pl.DeviceIdType.MESH
USED = (0, 2, 3, 4, 5)
PLANES = 32
CHUNKS = 4


def split(a, axis):
    hi = a.astype(BF16)
    lo = (a - hi.astype(F32)).astype(BF16)
    return jnp.concatenate([hi, lo], axis=axis)


def source_index(kind, length):
    return {2: length - 2, 3: length - 1, 4: 0, 5: 1}[kind]


def selector(length):
    kind = lax.broadcasted_iota(jnp.int32, (8, length), 0)
    at = lax.broadcasted_iota(jnp.int32, (8, length), 1)
    pick = kind == 0
    for k in (2, 3, 4, 5):
        pick = pick | ((kind == k) & (at == source_index(k, length)))
    one = jnp.where(pick, 1.0, 0.0).astype(BF16)
    return jnp.concatenate([one, one], axis=1)


def z_sources(rows):
    return lax.dot_general(
        selector(rows.shape[1]),
        split(rows, 1),
        (((1,), (1,)), ((), ())),
        preferred_element_type=F32,
    )


class Exchange:
    def __init__(self, send, recv):
        self.send, self.recv, self.count = send, recv, 0

    def start(self, axis, shift, src, dst):
        n, me = lax.axis_size(axis), lax.axis_index(axis)
        at = self.count
        self.count += 1
        copy = pltpu.make_async_remote_copy(
            src_ref=src,
            dst_ref=dst,
            send_sem=self.send.at[at],
            recv_sem=self.recv.at[at],
            device_id={axis: lax.rem(me + shift + n, n)},
            device_id_type=MESH,
        )
        sends = (me + shift >= 0) & (me + shift < n)
        receives = (me - shift >= 0) & (me - shift < n)
        pl.when(sends)(copy.start)
        return sends, receives, copy

    def layers(self, axis, src, carry, halo):
        out = []
        n = lax.axis_size(axis)
        if n > 1:
            out.append(self.start(axis, 1, src.at[pl.ds(2, 2)], halo.at[pl.ds(0, 2)]))
            out.append(self.start(axis, -1, src.at[pl.ds(4, 2)], halo.at[pl.ds(2, 2)]))
        for d in range(1, n):
            out.append(self.start(axis, d, src.at[pl.ds(0, 1)], carry.at[pl.ds(d - 1, 1)]))
        return out

    def whole(self, axis, src, slots):
        n = lax.axis_size(axis)
        out = [self.start(axis, d, src, slots.at[d - 1]) for d in range(1, n)]
        if n > 1:
            out.append(self.start(axis, -1, src, slots.at[n - 1]))
        return out


def arrived(copies):
    for _, receives, copy in copies:
        pl.when(receives)(copy.wait_recv)


def sent(copies):
    for sends, _, copy in copies:
        pl.when(sends)(copy.wait_send)


def carry_total(carry, n):
    total = carry[0]
    for d in range(1, n - 1):
        total = total + carry[d]
    return total


def put_layers(out_ref, carry, halo, n):
    out_ref[0] = carry_total(carry, n)
    out_ref[1] = jnp.zeros_like(out_ref[1])
    for k in range(4):
        out_ref[2 + k] = halo[k]
    for k in (6, 7):
        out_ref[k] = jnp.zeros_like(out_ref[k])


def combined(slots, n, kind):
    total = slots[0]
    for d in range(1, n - 1):
        total = total + slots[d]
    zero = jnp.zeros_like(total)
    result = jnp.where(kind == 0, total, zero)
    result = jnp.where((kind == 2) | (kind == 3), slots[0], result)
    return jnp.where((kind == 4) | (kind == 5), slots[n - 1], result)


def exchange_kernel(
    volume, w_ref,
    sum_out, box_out, x_out, y_out, xy_out, z_out, z1_out, z2_out,
    v, grid_z, tall, x_src, y_src, z_src, s_src, zx_src, corner, xx_src, corner_x, z1_src, z2_src,
    xc, xh, yc, yh, zc, zh, sc, sh, small, zxc, zxh, corner_y_in, xxc, xxh, corner_x_in,
    z1c, z1h, z2c, z2h, local, send, recv,
):
    sizes = {a: lax.axis_size(a) for a in ("gx", "gy", "gz")}
    nx, ny, nz = sizes["gx"], sizes["gy"], sizes["gz"]
    cx, cy, cz = v.shape
    part = cx // CHUNKS
    loads = []
    for c in range(CHUNKS):
        at = pl.ds(c * part, part)
        loads.append(pltpu.make_async_copy(volume.at[at], v.at[at], local.at[c]))
        loads[-1].start()
    for ref in (xc, xh, yc, yh, zc, zh, sc, sh, zxc, zxh, corner_y_in, xxc, xxh, corner_x_in,
                z1c, z1h, z2c, z2h):
        ref[...] = jnp.zeros_like(ref)
    barrier = pltpu.get_barrier_semaphore()
    for axis, n in sizes.items():
        me = lax.axis_index(axis)
        for d in range(1, n):
            pl.semaphore_signal(
                barrier, inc=1, device_id={axis: lax.rem(me + d, n)}, device_id_type=MESH
            )

    tall[:, pl.ds(0, 8), :] = jnp.zeros((part, 8, cz), F32)
    tall[:, pl.ds(8 + cy, 8), :] = jnp.zeros((part, 8, cz), F32)
    x_src[...] = jnp.zeros_like(x_src)
    s_src[...] = jnp.zeros_like(s_src)
    total = None
    for c in range(CHUNKS):
        at = pl.ds(c * part, part)
        loads[c].wait()
        planes = v[at]
        partial = jnp.sum(planes, axis=0)
        total = partial if total is None else total + partial
        y_src[0, at, :] = jnp.sum(planes, axis=1)
        for k in (2, 3, 4, 5):
            y_src[k, at, :] = planes[:, source_index(k, cy), :]
    x_src[0] = total
    for k in (2, 3, 4, 5):
        x_src[k] = v[source_index(k, cx)]
    pl.semaphore_wait(barrier, nx + ny + nz - 3)

    ex = Exchange(send, recv)
    to_y = ex.layers("gy", y_src, yc, yh)
    to_x = ex.layers("gx", x_src, xc, xh)
    planes = x_src[...]
    for k in USED:
        rows = jnp.sum(planes, axis=1) if k == 0 else planes[:, source_index(k, cy), :]
        s_src[k, pl.ds(0, 8), :] = rows
    zero = jnp.zeros((64, cz), F32)
    rows = [y_src[k] for k in USED] + [planes[:6].reshape(6 * cy, cz)]
    rows += [s_src[:, k, :] for k in range(8)] + [zero]
    found = z_sources(jnp.concatenate(rows, axis=0))
    for at, k in enumerate(USED):
        s_src[k, pl.ds(8, 8), :] = found[:, at * 128 : (at + 1) * 128]
    for k in range(3):
        zx_src[k] = found[:, (5 + k) * 128 : (6 + k) * 128]
    corner[0] = found[:, 8 * 128 : 9 * 128]
    to_y += ex.layers("gy", s_src, sc, sh)
    to_y += ex.whole("gy", corner, corner_y_in)
    to_x.append(ex.start("gx", 1, zx_src.at[pl.ds(1, 1)], zxh.at[pl.ds(0, 1)]))
    to_x.append(ex.start("gx", -1, zx_src.at[pl.ds(2, 1)], zxh.at[pl.ds(1, 1)]))
    for d in range(1, nx):
        to_x.append(ex.start("gx", d, zx_src.at[pl.ds(0, 1)], zxc.at[pl.ds(d - 1, 1)]))

    blocks = part * cy // 128
    for c in range(CHUNKS):
        found = z_sources(v[pl.ds(c * part, part)].reshape(part * cy, cz))
        z_src[:, pl.ds(c * blocks, blocks), :] = found.reshape(8, blocks, 128)
    to_z = ex.layers("gz", z_src, zc, zh)

    def own_sums(c):
        at = pl.ds(c * part, part)
        rows = split(v[at].reshape(part * cy, cz), 1)
        grid_z[...] = jnp.dot(rows, w_ref[...], preferred_element_type=F32)
        row = lax.broadcasted_iota(jnp.int32, (1, 8, cz), 1)
        tiles = grid_z[:, pl.ds(0, cz)].reshape(part * cy // 8, 8, cz)
        for step in (1, 2, 4):
            tiles = tiles + jnp.where(row >= step, pltpu.roll(tiles, step, 1), 0.0)
        tiles = tiles.reshape(part, cy // 8, 8, cz)
        start = None
        for k in range(cy // 8):
            now = tiles[:, k] if k == 0 else tiles[:, k] + start
            sum_out[at, pl.ds(8 * k, 8), :] = now
            start = now[:, 7:8, :]
        main = grid_z[:, pl.ds(cz, cz)].reshape(part, cy, cz)
        tall[:, pl.ds(8, cy), :] = main
        for d in (6, 7, 9, 10):
            main = main + tall[:, pl.ds(d, cy), :]
        box_out[at] = main

    lane = lax.broadcasted_iota(jnp.int32, (1, 8, 128), 2)
    arrived(to_y)
    put_layers(small, sc, sh, ny)
    for k in range(8):
        xx_src[k] = small[:, k, :]
        z1_src[k] = small[:, 8 + k, :]
    corner_x[...] = combined(corner_y_in, ny, lax.rem(lane, 8))
    to_x += ex.layers("gx", xx_src, xxc, xxh)
    to_x += ex.whole("gx", corner_x, corner_x_in)
    to_z += ex.layers("gz", z1_src, z1c, z1h)
    put_layers(y_out, yc, yh, ny)
    for c in range(CHUNKS // 2):
        own_sums(c)

    arrived(to_x)
    pairs = [carry_total(zxc, nx), zxh[0], zxh[1], combined(corner_x_in, nx, lane // 8)[0]]
    for k in range(8):
        rows = [p[k : k + 1] for p in pairs] + [jnp.zeros((4, 128), F32)]
        z2_src[k] = jnp.concatenate(rows, axis=0)
    to_z += ex.layers("gz", z2_src, z2c, z2h)
    put_layers(x_out, xc, xh, nx)
    put_layers(xy_out, xxc, xxh, nx)

    for c in range(CHUNKS // 2, CHUNKS):
        own_sums(c)
    arrived(to_z)
    put_layers(z_out, zc, zh, nz)
    put_layers(z1_out, z1c, z1h, nz)
    put_layers(z2_out, z2c, z2h, nz)
    sent(to_y + to_x + to_z)


def z_weights(nz):
    rows = lax.broadcasted_iota(jnp.int32, (nz, nz), 0)
    cols = lax.broadcasted_iota(jnp.int32, (nz, nz), 1)
    lower = jnp.where(rows <= cols, 1.0, 0.0).astype(BF16)
    band = jnp.where(jnp.abs(rows - cols) <= 2, 1.0, 0.0).astype(BF16)
    half = jnp.concatenate([lower, band], axis=1)
    kind = lax.broadcasted_iota(jnp.int32, (8, nz), 0)
    at = lax.broadcasted_iota(jnp.int32, (8, nz), 1)
    add = (kind == 2) & (at == 0)
    add |= (kind == 3) & (at <= 1)
    add |= (kind == 4) & (at >= nz - 2)
    add |= (kind == 5) & (at == nz - 1)
    edge = jnp.concatenate(
        [jnp.where(kind == 0, 1.0, 0.0).astype(BF16), jnp.where(add, 1.0, 0.0).astype(BF16)], axis=1
    )
    return jnp.concatenate([half, half], axis=0), jnp.concatenate([edge, edge], axis=0)


def y_weights(ny):
    rows = lax.broadcasted_iota(jnp.int32, (128, 128), 0)
    cols = lax.broadcasted_iota(jnp.int32, (128, 128), 1)
    same = rows // ny == cols // ny
    lower = jnp.where(same & (rows <= cols), 1.0, 0.0).astype(BF16)
    band = jnp.where(same & (jnp.abs(rows - cols) <= 2), 1.0, 0.0).astype(BF16)
    half = jnp.concatenate([lower, band], axis=1)
    return jnp.concatenate([half, half], axis=0)


def along_z(rows, edges, w_ref, e_ref):
    main = jnp.dot(split(rows, 1), w_ref[...], preferred_element_type=F32)
    return main + lax.dot_general(
        split(edges, 0), e_ref[...], (((0,), (0,)), ((), ())), preferred_element_type=F32
    )


def final_kernel(
    ny, nz, scale,
    sum_ref, own_ref, x_ref, y_ref, xy_ref, z_ref, z1_ref, z2_ref, w_ref, e_ref, yw_ref,
    prefix_ref, box_ref,
    edge_z, edge_y, rows_y, plane_z, corner_z, run, tall, boxed,
):
    i, steps = pl.program_id(0), pl.num_programs(0)
    count = y_ref.shape[1]
    blocks = PLANES * ny // 128
    zrows = z_ref.shape[0] // 8

    def y_prefix(piece, start):
        row = lax.broadcasted_iota(jnp.int32, (1, 8, nz), 1)
        c = piece.reshape(ny // 8, 8, nz)
        for step in (1, 2, 4):
            c = c + jnp.where(row >= step, pltpu.roll(c, step, 1), 0.0)
        out = []
        for k in range(ny // 8):
            out.append(c[k] + start)
            start = out[-1][7:8]
        return jnp.concatenate(out, axis=0)

    def y_box(slot, piece, before, after):
        tall[slot, pl.ds(8, ny), :] = piece
        tall[slot, pl.ds(6, 1), :] = before[0]
        tall[slot, pl.ds(7, 1), :] = before[1]
        tall[slot, pl.ds(8 + ny, 1), :] = after[0]
        tall[slot, pl.ds(9 + ny, 1), :] = after[1]
        total = piece
        for d in (6, 7, 9, 10):
            total = total + tall[slot, pl.ds(d, ny), :]
        return total

    def row_of(k, x, part):
        return corner_z[pl.ds(x * 8 + k, 1), pl.ds(part * nz, nz)]

    @pl.when(i == 0)
    def _():
        found = jnp.dot(split(z_ref[...], 1), yw_ref[...], preferred_element_type=F32)
        edge_y[pl.ds(0, zrows), :] = found[:zrows, :128]
        edge_y[pl.ds(zrows, 7 * zrows), :] = found[zrows:, 128:]
        for k in USED:
            rows_y[k] = along_z(y_ref[k], z1_ref[:, k, :], w_ref, e_ref)
        corner_z[...] = along_z(xy_ref[...].reshape(64, nz), z2_ref[:, 3, :][:, :64], w_ref, e_ref)
        edges = jnp.concatenate([z2_ref[:, k, :] for k in range(3)], axis=1)
        plane_z[...] = along_z(x_ref[:6].reshape(6 * ny, nz), edges, w_ref, e_ref)
        run[...] = y_prefix(plane_z[pl.ds(0, ny), pl.ds(0, nz)], row_of(0, 0, 0))
        for k, to in ((2, 0), (3, 1), (4, count + 2), (5, count + 3)):
            boxed[to] = y_box(
                k % 4,
                plane_z[pl.ds(k * ny, ny), pl.ds(nz, nz)],
                [row_of(t, k, 1) for t in (2, 3)],
                [row_of(t, k, 1) for t in (4, 5)],
            )

    @pl.when(i < steps - 1)
    def _():
        edges = jnp.concatenate(
            [edge_y[pl.ds(i * blocks + b, 8, stride=zrows), :] for b in range(blocks)], axis=1
        )
        edge_z[...] = lax.dot_general(
            split(edges, 0), e_ref[...], (((0,), (0,)), ((), ())), preferred_element_type=F32
        )
        running = run[...]
        here = pl.ds(pl.multiple_of(i * PLANES, PLANES), PLANES)
        starts = rows_y[0, here, pl.ds(0, nz)]
        b2, b1, a1, a2 = (rows_y[t, here, pl.ds(nz, nz)] for t in (2, 3, 4, 5))
        below, above = b2 + b1, a1 + a2
        row = lax.broadcasted_iota(jnp.int32, (8, nz), 0)
        for p in range(PLANES):
            x = i * PLANES + p
            at = pl.ds(p * ny, ny)
            running = running + (sum_ref[x] + edge_z[at, pl.ds(0, nz)] + starts[p : p + 1])
            prefix_ref[at, :] = running * F32(scale)
            own = own_ref[x] + edge_z[at, pl.ds(nz, nz)]
            low = jnp.where(row == 0, below[p : p + 1], jnp.where(row == 1, b1[p : p + 1], 0.0))
            top = jnp.where(row == 7, above[p : p + 1], jnp.where(row == 6, a1[p : p + 1], 0.0))
            boxed[x + 2, pl.ds(0, 8), :] = own[:8] + low
            boxed[x + 2, pl.ds(8, ny - 16), :] = own[8 : ny - 8]
            boxed[x + 2, pl.ds(ny - 8, 8), :] = own[ny - 8 :] + top
        run[...] = running

    @pl.when(i > 0)
    def _():
        for p in range(PLANES):
            x = (i - 1) * PLANES + p
            total = boxed[x]
            for d in range(1, 5):
                total = total + boxed[x + d]
            box_ref[pl.ds(p * ny, ny), :] = total * F32(1.0 / math.sqrt(125.0))


def per_device(volume):
    cx, cy, cz = volume.shape
    nx, ny, nz = (lax.axis_size(a) for a in ("gx", "gy", "gz"))
    steps = cx // PLANES
    rows = PLANES * cy
    zrows = cx * cy // 128

    def of(*shape):
        return jax.ShapeDtypeStruct(shape, F32)

    vmem = pl.BlockSpec(memory_space=pltpu.VMEM)
    weights, edge_weights = z_weights(cz)
    copies = 8 * (nx + ny + nz) + 4
    lx, ly, lz = (max(n - 1, 1) for n in (nx, ny, nz))
    row = (8, 128)
    faces = [(cx, cy, cz), (cx, cy, cz), (8, cy, cz), (8, cx, cz), (8, 8, cz), (8, zrows, 128), (8, 8, cx), (8, 8, 128)]
    buffers = [
        (cx, cy, cz), (cx // CHUNKS * cy, 2 * cz), (cx // CHUNKS, cy + 16, cz),
        (8, cy, cz), (8, cx, cz), (8, zrows, 128), (8, 16, 128), (3, *row),
        (1, *row), (8, *row), (1, *row), (8, *row), (8, *row),
        (lx, cy, cz), (4, cy, cz), (ly, cx, cz), (4, cx, cz), (lz, zrows, 128), (4, zrows, 128),
        (ly, 16, 128), (4, 16, 128), (8, 16, 128), (lx, *row), (2, *row), (ny, 1, *row),
        (lx, *row), (4, *row), (nx, 1, *row),
        (lz, *row), (4, *row), (lz, *row), (4, *row),
    ]
    own_sum, own_box, x, y, xy, z, z1, z2 = pl.pallas_call(
        exchange_kernel,
        in_specs=[pl.BlockSpec(memory_space=pltpu.HBM), vmem],
        out_specs=[vmem] * 8,
        out_shape=[of(*s) for s in faces],
        scratch_shapes=[pltpu.VMEM(s, F32) for s in buffers]
        + [pltpu.SemaphoreType.DMA((CHUNKS,))]
        + [pltpu.SemaphoreType.DMA((copies,)), pltpu.SemaphoreType.DMA((copies,))],
        compiler_params=pltpu.CompilerParams(
            collective_id=0, has_side_effects=True, vmem_limit_bytes=44 * 1024 * 1024
        ),
    )(volume, weights)
    z = z.reshape(8 * zrows, 128)

    scale = 1.0 / math.sqrt(cx * nx * cy * ny * cz * nz)
    prefix, box = pl.pallas_call(
        functools.partial(final_kernel, cy, cz, scale),
        grid=(steps + 1,),
        in_specs=[vmem] * 11,
        out_specs=[
            pl.BlockSpec((rows, cz), lambda i: (jnp.minimum(i, steps - 1), 0)),
            pl.BlockSpec((rows, cz), lambda i: (jnp.maximum(i - 1, 0), 0)),
        ],
        out_shape=[of(cx * cy, cz), of(cx * cy, cz)],
        scratch_shapes=[
            pltpu.VMEM((rows, 2 * cz), F32),
            pltpu.VMEM((8 * zrows, 128), F32),
            pltpu.VMEM((6, cx, 2 * cz), F32),
            pltpu.VMEM((6 * cy, 2 * cz), F32),
            pltpu.VMEM((64, 2 * cz), F32),
            pltpu.VMEM((cy, cz), F32),
            pltpu.VMEM((4, cy + 16, cz), F32),
            pltpu.VMEM((cx + 4, cy, cz), F32),
        ],
        compiler_params=pltpu.CompilerParams(vmem_limit_bytes=24 * 1024 * 1024),
    )(own_sum, own_box, x, y, xy, z, z1, z2, weights, edge_weights, y_weights(cy))
    return prefix.reshape(cx, cy, cz), box.reshape(cx, cy, cz)


def solution(mesh):
    return jax.shard_map(
        per_device,
        mesh=mesh,
        in_specs=(P("gx", "gy", "gz"),),
        out_specs=(P("gx", "gy", "gz"), P("gx", "gy", "gz")),
        check_vma=False,
    )
```
